128 devices in a mesh: node: 16 (over z, y), data: 8 (over x, core).
Axes of the slice: x: 4, y: 4, z: 4, core: 2. Of those that a mesh axis runs over, the one named last changes fastest.
Arguments:
- tokens: bfloat16 [131072, 768], P(('node', 'data'))
- grad_out: bfloat16 [131072, 768], P(('node', 'data'))
- weights: bfloat16 [8, 768, 768], replicated
- a_old: float32 [8, 768, 768], replicated
- s_old: float32 [8, 768, 768], replicated
- a_inv: float32 [8, 768, 768], replicated
- s_inv: float32 [8, 768, 768], replicated
Outputs:
- output 1: float32 [8, 768, 768], replicated
- output 2: float32 [8, 768, 768], replicated
- output 3: float32 [8, 768, 768], replicated
All inputs are finite; a program needn't handle non-finite values.
Results may differ from the reference program's by a relative error of at most 0.00169187.
Values are sent between devices in bfloat16 or wider.
A program may use at most 1 GiB of HBM per device.

```python
import jax
import jax.numpy as jnp
from jax import lax

D = 768
LAYERS = 8
TOKENS_DEV = 1024
SHARDS = 128
TOKENS_ALL = SHARDS * TOKENS_DEV
FACTOR_DECAY = 0.8
GELU_SCALE = 0.7978845608028654
GELU_CUBIC = 0.044715


def spd_draw(rng_key):
    key_diag, key_low = jax.random.split(rng_key)
    diagonal = jax.random.uniform(key_diag, (LAYERS, D), jnp.float32, 0.5, 1.5)
    low_part = jax.random.normal(key_low, (LAYERS, D, 64), jnp.float32) * D ** -0.5
    low_sq = jnp.einsum('lir,ljr->lij', low_part, low_part)
    return low_sq + diagonal[:, :, None] * jnp.eye(D, dtype=jnp.float32)


def draw_side(key_noise, key_scale, key_shift, shift_size):
    noise = jax.random.normal(key_noise, (SHARDS, TOKENS_DEV, D), jnp.float32)
    shard_scale = jax.random.uniform(key_scale, (SHARDS, 1, 1), jnp.float32, 0.5, 1.5)
    shard_shift = shift_size * jax.random.normal(key_shift, (SHARDS, 1, D), jnp.float32)
    return (noise * shard_scale + shard_shift).reshape(TOKENS_ALL, D).astype(jnp.bfloat16)


def setup_inputs(seed: int = 0) -> dict:
    keys = jax.random.split(jax.random.key(seed), 11)
    tokens = draw_side(keys[0], keys[1], keys[2], 0.7)
    grad_out = draw_side(keys[3], keys[4], keys[5], 0.7)
    weights = (1.5 * D ** -0.5 * jax.random.normal(keys[6], (LAYERS, D, D), jnp.float32)).astype(jnp.bfloat16)
    return {'tokens': tokens, 'grad_out': grad_out, 'weights': weights, 'a_old': spd_draw(keys[7]), 's_old': spd_draw(keys[8]), 'a_inv': spd_draw(keys[9]), 's_inv': spd_draw(keys[10])}


def gelu_value(pre_act):
    pre_f = pre_act.astype(jnp.float32)
    return 0.5 * pre_f * (1.0 + jnp.tanh(GELU_SCALE * (pre_f + GELU_CUBIC * pre_f * pre_f * pre_f)))


def gelu_slope(pre_act):
    pre_f = pre_act.astype(jnp.float32)
    tanh_val = jnp.tanh(GELU_SCALE * (pre_f + GELU_CUBIC * pre_f * pre_f * pre_f))
    return 0.5 * (1.0 + tanh_val) + 0.5 * pre_f * (1.0 - tanh_val * tanh_val) * GELU_SCALE * (1.0 + 3.0 * GELU_CUBIC * pre_f * pre_f)


def shard_terms(tok_rows, dout_rows, weights):
    hidden = [tok_rows]
    pre_list = []
    for layer in range(LAYERS - 1):
        pre_act = jnp.dot(hidden[layer], weights[layer], preferred_element_type=jnp.float32).astype(jnp.bfloat16)
        pre_list.append(pre_act)
        hidden.append(gelu_value(pre_act).astype(jnp.bfloat16))
    w_parts = []
    a_parts = []
    s_parts = []
    grad_h = dout_rows
    for layer in reversed(range(LAYERS)):
        if layer == LAYERS - 1:
            grad_pre = grad_h
        else:
            grad_pre = (grad_h.astype(jnp.float32) * gelu_slope(pre_list[layer])).astype(jnp.bfloat16)
        w_parts.append(jnp.dot(hidden[layer].T, grad_pre, preferred_element_type=jnp.float32))
        a_parts.append(jnp.dot(hidden[layer].T, hidden[layer], preferred_element_type=jnp.float32))
        s_parts.append(jnp.dot(grad_pre.T, grad_pre, preferred_element_type=jnp.float32))
        if layer > 0:
            grad_h = jnp.dot(grad_pre, weights[layer].T, preferred_element_type=jnp.float32).astype(jnp.bfloat16)
    return (jnp.stack(w_parts[::-1]), jnp.stack(a_parts[::-1]), jnp.stack(s_parts[::-1]))


def reference(tokens, grad_out, weights, a_old, s_old, a_inv, s_inv):
    tok_blocks = tokens.reshape(SHARDS, TOKENS_DEV, D)
    dout_blocks = grad_out.reshape(SHARDS, TOKENS_DEV, D)

    def accumulate(totals, block_pair):
        pieces = shard_terms(block_pair[0], block_pair[1], weights)
        return tuple(total + piece for total, piece in zip(totals, pieces)), None

    zero_stack = jnp.zeros((LAYERS, D, D), jnp.float32)
    sums = lax.scan(accumulate, (zero_stack, zero_stack, zero_stack), (tok_blocks, dout_blocks))[0]
    grad_w = sums[0] / TOKENS_ALL
    a_cur = sums[1] / TOKENS_ALL
    s_cur = sums[2] / TOKENS_ALL
    a_new = FACTOR_DECAY * a_old + (1.0 - FACTOR_DECAY) * a_cur
    s_new = FACTOR_DECAY * s_old + (1.0 - FACTOR_DECAY) * s_cur
    left = jnp.einsum('lij,ljk->lik', a_inv.astype(jnp.float32), grad_w.astype(jnp.float32))
    update = jnp.einsum('lij,ljk->lik', left, s_inv.astype(jnp.float32))
    return (update, a_new, s_new)
```

```python
import functools

import jax
import jax.numpy as jnp
from jax import lax
from jax.experimental import pallas as pl
from jax.experimental.pallas import tpu as pltpu
from jax.sharding import PartitionSpec as P

FACTOR_DECAY = 0.8
GELU_SCALE = 0.7978845608028654
GELU_CUBIC = 0.044715
MESH = pl.DeviceIdType.MESH
W = 768
ROUNDS = 8
NX, NR, NG = 3, 3, 4
PERIODS = ROUNDS + 5
DIAG_PERIOD = 1
F32 = jnp.float32


def comm_kernel(u_ref, ainv_ref, sinv_ref, diag_ref, packed_ref, upd_ref, dsum_ref,
                X, R, G, D, INV, UPD, MS, ML,
                rsem, ssem, lsem, dsend, drecv, isem, osem, osend, orecv, msend, mrecv, mloc):
    node, data = lax.axis_index('node'), lax.axis_index('data')
    core = lax.rem(data, 2)
    coord = [data // 2, lax.rem(node, 4), node // 4]

    def device(axis, delta):
        c = list(coord)
        c[axis] = lax.rem(c[axis] + delta + 4, 4)
        return (c[2] * 4 + c[1], c[0] * 2 + core)

    partner = (node, data + 1 - 2 * core)

    barrier = pltpu.get_barrier_semaphore()
    peers = [partner] + [device(a, d) for a in range(3) for d in (1, 2, 3)]
    for dev in peers:
        pl.semaphore_signal(barrier, inc=1, device_id=dev, device_id_type=MESH)
    pl.semaphore_wait(barrier, len(peers))

    def mo(v, m):
        return pl.multiple_of(v, m)

    def send(src, dst, s, r, dev):
        pltpu.make_async_remote_copy(src_ref=src, dst_ref=dst, send_sem=s, recv_sem=r, device_id=dev, device_id_type=MESH).start()

    def wait(ref, sem):
        pltpu.make_async_copy(ref, ref, sem).wait()

    def is_update(p):
        return (p == 2) | (p == 3) | (p == 5) | (p == 6)

    def layer_of(p):
        return 7 - 2 * jnp.where(p > 4, p - 3, p - 2) - core

    def packed_of(p):
        return 2 * jnp.where(p < 2, p, jnp.where(p == 4, 2, 3)) + core

    def place(k, s):
        return coord[(k + s) % 3]

    def region(p, k, s, j, half, slots=NX):
        row = mo(lax.rem(p, slots) * W, W) + 256 * k
        if s == 0:
            row = row + 64 * j
            n, col, m = 64, 0, W
        elif s == 1:
            row = row + 64 * place(k, 0) + 16 * j
            n, col, m = 16, 0, W
        else:
            row = row + 64 * place(k, 0) + 16 * place(k, 1) + 8 * (j // 2)
            n, col, m = 8, 384 * lax.rem(j, 2), 384
        if half is not None:
            if s < 2:
                n //= 2
                row = row + half * n
            else:
                col, m = (col, 128) if half == 0 else (col + 128, 256)
        row = mo(row, 8)
        if s < 2:
            return pl.ds(row, n), pl.ds(0, W)
        return pl.ds(row, n), pl.ds(mo(col, 128), m)

    def landing(p, k, s, what, side, half):
        row = mo(lax.rem(p, NR) * W, W) + 256 * k
        if s < 2:
            h = (32, 8)[s]
            row = row + (0, 192)[s]
            if what == 0:
                if side is None:
                    return pl.ds(mo(row, 8), 2 * h), pl.ds(0, W)
                return pl.ds(mo(row + side * h, 8), h), pl.ds(0, W)
            row = row + 2 * h
            if side is None:
                return pl.ds(mo(row, 8), 4 * h), pl.ds(0, W)
            row = row + side * 2 * h
            if half is None:
                return pl.ds(mo(row, 8), 2 * h), pl.ds(0, W)
            return pl.ds(mo(row + half * h, 8), h), pl.ds(0, W)
        row = mo(row + 240 + 8 * what, 8)
        if what == 0:
            if side is None:
                return pl.ds(row, 8), pl.ds(0, 384)
            return pl.ds(row, 8), (pl.ds(0, 128) if side == 0 else pl.ds(128, 256))
        if side is None:
            return pl.ds(row, 8), pl.ds(0, W)
        if half is None:
            return pl.ds(row, 8), pl.ds(384 * side, 384)
        return pl.ds(row, 8), (pl.ds(384 * side, 128) if half == 0 else pl.ds(384 * side + 128, 256))

    def neighbours(k, s):
        a = (k + s) % 3
        return place(k, s), device(a, 1), device(a, -1)

    def around(i):
        return lax.rem(i + 1, 4), lax.rem(i + 3, 4), lax.rem(i + 2, 4)

    def rs(p, k, s, w):
        return rsem.at[lax.rem(p, NR), (k * 3 + s) * 4 + w]

    def ss(p, k, s, w):
        return ssem.at[lax.rem(p, NR), (k * 3 + s) * 4 + w]

    def add(dst, src):
        X[dst] = X[dst] + R[src]

    def scatter_a(p, k, s):
        i, plus, minus = neighbours(k, s)
        jp, jm, j2 = around(i)
        fwd, blk, sa = rs(p, k, s, 0), rs(p, k, s, 1), ss(p, k, s, 0)
        send(X.at[region(p, k, s, j2, 0)], R.at[landing(p, k, s, 0, 0, None)], sa, fwd, minus)
        send(X.at[region(p, k, s, j2, 1)], R.at[landing(p, k, s, 0, 1, None)], sa, fwd, plus)
        send(X.at[region(p, k, s, jm, 1)], R.at[landing(p, k, s, 1, 0, 1)], sa, blk, minus)
        send(X.at[region(p, k, s, jp, 0)], R.at[landing(p, k, s, 1, 1, 0)], sa, blk, plus)

    def scatter_b(p, k, s):
        i, plus, minus = neighbours(k, s)
        jp, jm, _ = around(i)
        blk, sb = rs(p, k, s, 1), ss(p, k, s, 1)
        wait(R.at[landing(p, k, s, 0, None, None)], rs(p, k, s, 0))
        add(region(p, k, s, jm, 0), landing(p, k, s, 0, 0, None))
        send(X.at[region(p, k, s, jm, 0)], R.at[landing(p, k, s, 1, 0, 0)], sb, blk, minus)
        add(region(p, k, s, jp, 1), landing(p, k, s, 0, 1, None))
        send(X.at[region(p, k, s, jp, 1)], R.at[landing(p, k, s, 1, 1, 1)], sb, blk, plus)

    def scatter_c(p, k, s):
        i = place(k, s)
        wait(R.at[landing(p, k, s, 1, None, None)], rs(p, k, s, 1))
        mine = region(p, k, s, i, None)
        value = X[mine] + (R[landing(p, k, s, 1, 0, None)] + R[landing(p, k, s, 1, 1, None)])
        if s < 2:
            X[mine] = value
        else:
            G[region(p, k, s, i, None, NG)] = value

    def gather_a(p, k, s):
        i, plus, minus = neighbours(k, s)
        mine = G.at[region(p, k, s, i, None, NG)]
        send(mine, mine, ss(p, k, s, 2), rs(p, k, s, 2), plus)
        send(mine, mine, ss(p, k, s, 2), rs(p, k, s, 2), minus)

    def gather_b(p, k, s):
        i, plus, minus = neighbours(k, s)
        jp, jm, _ = around(i)
        wait(R.at[landing(p, k, s, 1, None, None)], rs(p, k, s, 2))
        from_minus, from_plus = G.at[region(p, k, s, jm, 0, NG)], G.at[region(p, k, s, jp, 1, NG)]
        send(from_minus, from_minus, ss(p, k, s, 3), rs(p, k, s, 3), plus)
        send(from_plus, from_plus, ss(p, k, s, 3), rs(p, k, s, 3), minus)

    def gather_c(p, k, s):
        wait(R.at[landing(p, k, s, 0, None, None)], rs(p, k, s, 3))

    def colours(f, p, s):
        for k in range(3):
            f(p, k, s)

    def gslot(p):
        return G.at[pl.ds(mo(lax.rem(p, NG) * W, W), W)]

    def xslot(p):
        return X.at[pl.ds(mo(lax.rem(p, NX) * W, W), W)]

    def unit(ref, index):
        return ref.at[pl.ds(mo(index * W, W), W)]

    def dslot(p):
        return D.at[pl.ds(mo(lax.rem(p, 2) * W, W), W)]

    def step0(p):
        pltpu.make_async_copy(unit(u_ref, 2 * p + core), xslot(p), lsem.at[lax.rem(p, 2)]).start()
        send(unit(u_ref, 2 * p + 1 - core), dslot(p), dsend.at[lax.rem(p, 2)], drecv.at[lax.rem(p, 2)], partner)

    def step1(p):
        wait(xslot(p), lsem.at[lax.rem(p, 2)])
        wait(dslot(p), drecv.at[lax.rem(p, 2)])

        def some(c, carry):
            a = pl.ds(mo(lax.rem(p, NX) * W + c * 64, 64), 64)
            X[a, :] = X[a, :] + D[pl.ds(mo(lax.rem(p, 2) * W + c * 64, 64), 64), :]
            return carry
        lax.fori_loop(0, 12, some, 0)
        colours(scatter_a, p, 0)

    def step2(p):
        colours(scatter_b, p, 0)
        wait(dslot(p), dsend.at[lax.rem(p, 2)])

    def step3(p):
        colours(scatter_c, p, 0)
        colours(scatter_a, p, 1)

    def step4(p):
        colours(scatter_b, p, 1)

    def step5(p):
        colours(scatter_c, p, 1)
        colours(scatter_a, p, 2)

    def step6(p):
        colours(scatter_b, p, 2)

    def step7(p):
        colours(scatter_c, p, 2)
        colours(gather_a, p, 2)

    def step8(p):
        colours(gather_b, p, 2)
        for k in range(3):
            for s in range(3):
                wait(R.at[landing(p, k, s, 1, None, None)], ss(p, k, s, 0))
                wait(R.at[landing(p, k, s, 0, None, None)], ss(p, k, s, 1))

    def step9(p):
        colours(gather_c, p, 2)
        colours(gather_a, p, 1)

    def inverse(p, which):
        return INV.at[pl.ds(mo(lax.rem(p, 2) * (2 * W) + which * W, W), W)]

    def step10(p):
        colours(gather_b, p, 1)

        @pl.when(is_update(p))
        def _():
            l = layer_of(p)
            pltpu.make_async_copy(ainv_ref.at[l], inverse(p, 0), isem.at[lax.rem(p, 2), 0]).start()
            pltpu.make_async_copy(sinv_ref.at[l], inverse(p, 1), isem.at[lax.rem(p, 2), 1]).start()

    def step11(p):
        colours(gather_c, p, 1)
        colours(gather_a, p, 0)

    def step12(p):
        colours(gather_b, p, 0)

    def piece(p, part):
        @pl.when(is_update(p))
        def _():
            rows = 256 * part
            turn = lax.rem(p, 2)
            a = INV[pl.ds(mo(turn * (2 * W) + rows, 256), 256), :]
            g = G[pl.ds(mo(lax.rem(p, NG) * W, W), W), :]
            left = jnp.dot(a, g, precision=lax.Precision.HIGHEST, preferred_element_type=F32) * (1.0 / 131072.0)
            b = INV[pl.ds(mo(turn * (2 * W) + W, W), W), :]
            here = pl.ds(mo(turn * W + rows, 256), 256)
            UPD[here, :] = jnp.dot(left, b, precision=lax.Precision.HIGHEST, preferred_element_type=F32)
            out = upd_ref.at[layer_of(p), pl.ds(rows, 256)]
            pltpu.make_async_copy(UPD.at[here], out, osem.at[lax.rem(p, 2)]).start()
            send(UPD.at[here], out, osend.at[lax.rem(p, 2)], orecv.at[p], partner)

    def step13(p):
        colours(gather_c, p, 0)

        @pl.when(is_update(p))
        def _():
            wait(inverse(p, 0), isem.at[lax.rem(p, 2), 0])
            wait(inverse(p, 1), isem.at[lax.rem(p, 2), 1])

        @pl.when(jnp.logical_not(is_update(p)))
        def _():
            out = packed_ref.at[packed_of(p)]
            pltpu.make_async_copy(gslot(p), out, osem.at[lax.rem(p, 2)]).start()
            send(gslot(p), out, osend.at[lax.rem(p, 2)], orecv.at[p], partner)
        piece(p, 0)

    def step14(p):
        for k in range(3):
            for s in range(3):
                wait(R.at[landing(0, k, s, 1, None, None)], ss(p, k, s, 2))
                wait(R.at[landing(0, k, s, 0, None, None)], ss(p, k, s, 3))
        piece(p, 1)

    def step15(p):
        piece(p, 2)

    def step16(p):
        wait(xslot(p), osem.at[lax.rem(p, 2)])
        wait(xslot(p), osend.at[lax.rem(p, 2)])

    def step17(p):
        wait(xslot(p), orecv.at[p])

    steps = [step0, step1, step2, step3, step4, step5, step6, step7, step8, step9, step10, step11, step12, step13, step14, step15, step16, step17]
    slots = [(0, 6, 9, 3, 12, 15), (7, 10, 4, 1, 13, 16), (8, 5, 11, 2, 14, 17)]

    def ms(n):
        return pl.ds(8 * n, 8)

    def small_send(stage):
        if stage == 0:
            send(MS.at[ms(0)], ML.at[ms(0)], msend.at[0], mrecv.at[0], partner)
        else:
            for d in (1, 2, 3):
                n = 3 * stage - 3 + d
                send(MS.at[ms(stage)], ML.at[ms(n)], msend.at[n], mrecv.at[n], device(stage - 1, d))

    def small_take(stage):
        if stage == 0:
            wait(ML.at[ms(0)], mrecv.at[0])
            wait(ML.at[ms(0)], msend.at[0])
            MS[ms(1), :] = MS[ms(0), :] + ML[ms(0), :]
        else:
            n = 3 * stage - 3
            for d in (1, 2, 3):
                wait(ML.at[ms(n + d)], mrecv.at[n + d])
                wait(ML.at[ms(n + d)], msend.at[n + d])
            MS[ms(stage + 1), :] = (MS[ms(stage), :] + ML[ms(n + 2), :]) + (ML[ms(n + 1), :] + ML[ms(n + 3), :])

    def small0():
        load = pltpu.make_async_copy(diag_ref, MS.at[ms(0)], mloc.at[0])
        load.start()
        load.wait()
        small_send(0)

    def small4():
        small_take(3)
        store = pltpu.make_async_copy(MS.at[ms(4)], dsum_ref, mloc.at[1])
        store.start()
        store.wait()

    def small_mid(n):
        small_take(n - 1)
        small_send(n)

    small = [small0] + [functools.partial(small_mid, n) for n in (1, 2, 3)] + [small4]

    def period(t, carry):
        for sub in range(3):
            for n in slots[sub]:
                p = t - n // 3

                @pl.when((p >= 0) & (p < ROUNDS))
                def _(n=n, p=p):
                    steps[n](p)
            for n in range(5):
                if n % 3 == sub:
                    pl.when(t == DIAG_PERIOD + n // 3)(small[n])
        return carry

    lax.fori_loop(0, PERIODS, period, 0)


def reduce_units(units, a_inv, s_inv, diag):
    any_space = pl.BlockSpec(memory_space=pl.ANY)
    dma = pltpu.SemaphoreType.DMA
    return pl.pallas_call(
        comm_kernel,
        out_shape=(jax.ShapeDtypeStruct((8, W, W), F32), jax.ShapeDtypeStruct((8, W, W), F32), jax.ShapeDtypeStruct((8, W), F32)),
        in_specs=[any_space] * 4,
        out_specs=(any_space,) * 3,
        scratch_shapes=[
            pltpu.VMEM((NX * W, W), F32),
            pltpu.VMEM((NR * W, W), F32),
            pltpu.VMEM((NG * W, W), F32),
            pltpu.VMEM((2 * W, W), F32),
            pltpu.VMEM((4 * W, W), F32),
            pltpu.VMEM((2 * W, W), F32),
            pltpu.VMEM((40, W), F32),
            pltpu.VMEM((80, W), F32),
            dma((NR, 36)), dma((NR, 36)), dma((2,)), dma((2,)), dma((2,)), dma((2, 2)),
            dma((2,)), dma((2,)), dma((ROUNDS,)), dma((10,)), dma((10,)), dma((2,)),
        ],
        compiler_params=pltpu.CompilerParams(collective_id=0, has_side_effects=True, vmem_limit_bytes=62 * 1024 * 1024),
        name='reduce_units',
    )(units, a_inv, s_inv, diag)


def blend_kernel(first_row, p_ref, d_ref, old_ref, *refs):
    new_ref = refs[0] if len(refs) == 1 else refs[1]
    t, h = pl.program_id(0), pl.program_id(1)
    if len(refs) == 3:
        refs[2][...] = refs[0][...]
    block = 128
    for rb in range(W // block):
        rows = pl.ds(rb * block, block)
        here = p_ref[0, rows, :]
        turned = p_ref[0, :, rows].T
        r = lax.broadcasted_iota(jnp.int32, (block, W), 0) + rb * block
        c = lax.broadcasted_iota(jnp.int32, (block, W), 1)
        diag = d_ref[pl.ds(first_row + t, 1), :]
        first = jnp.where(r <= c, here, turned)
        second = jnp.where(r == c, diag, jnp.where(r < c, turned, here))
        value = jnp.where(h == 0, first, second) * (1.0 / 131072.0)
        new_ref[0, rows, :] = FACTOR_DECAY * old_ref[0, rows, :] + (1.0 - FACTOR_DECAY) * value


def blend(packed, dsum, old, first_row, pair_of, carried=None):
    mat = pl.BlockSpec((1, W, W), lambda t, h: (2 * pair_of(t) + h, 0, 0))
    in_specs = [pl.BlockSpec((1, W, W), lambda t, h: (first_row + t, 0, 0)), pl.BlockSpec((8, W), lambda t, h: (0, 0)), mat]
    shape = jax.ShapeDtypeStruct((8, W, W), F32)
    args = [packed, dsum, old]
    out_specs, out_shape = (mat,), (shape,)
    if carried is not None:
        in_specs.append(mat)
        args.append(carried)
        out_specs, out_shape = (mat, mat), (shape, shape)
    return pl.pallas_call(
        functools.partial(blend_kernel, first_row),
        grid=(4, 2),
        in_specs=in_specs,
        out_specs=out_specs,
        out_shape=out_shape,
        compiler_params=pltpu.CompilerParams(vmem_limit_bytes=60 * 1024 * 1024),
        name='blend',
    )(*args)


def gelu_value(pre_act):
    pre_f = pre_act.astype(F32)
    return 0.5 * pre_f * (1.0 + jnp.tanh(GELU_SCALE * (pre_f + GELU_CUBIC * pre_f * pre_f * pre_f)))


def gelu_slope(pre_act):
    pre_f = pre_act.astype(F32)
    tanh_val = jnp.tanh(GELU_SCALE * (pre_f + GELU_CUBIC * pre_f * pre_f * pre_f))
    return 0.5 * (1.0 + tanh_val) + 0.5 * pre_f * (1.0 - tanh_val * tanh_val) * GELU_SCALE * (1.0 + 3.0 * GELU_CUBIC * pre_f * pre_f)


def row_gram(left, right):
    return lax.dot_general(left, right, (((0,), (0,)), ((), ())), preferred_element_type=F32)


def solution(mesh):
    row_spec = P(('node', 'data'), None)
    full_spec = P()

    def per_device(tok, dout, w, a_prev, s_prev, a_pre, s_pre):
        layers = 8
        rows = lax.broadcasted_iota(jnp.int32, (W, W), 0)
        cols = lax.broadcasted_iota(jnp.int32, (W, W), 1)
        hidden = [tok]
        pre = []
        for l in range(layers - 1):
            z = jnp.dot(hidden[l], w[l], preferred_element_type=F32).astype(jnp.bfloat16)
            pre.append(z)
            hidden.append(gelu_value(z).astype(jnp.bfloat16))
        grads = [None] * layers
        dh = dout
        for l in reversed(range(layers)):
            g = dh if l == layers - 1 else (dh.astype(F32) * gelu_slope(pre[l])).astype(jnp.bfloat16)
            grads[l] = g
            if l > 0:
                dh = lax.dot_general(g, w[l], (((1,), (1,)), ((), ())), preferred_element_type=F32).astype(jnp.bfloat16)
        diags = []

        def pair(arrs, i):
            first, second = row_gram(arrs[i], arrs[i]), row_gram(arrs[i + 1], arrs[i + 1])
            diags.append(jnp.sum(jnp.where(rows == cols, second, 0.0), axis=0))
            return jnp.where(rows <= cols, first, second)

        def cross(l):
            return row_gram(hidden[l], grads[l])

        units = [pair(hidden, 0), pair(hidden, 2), pair(hidden, 4), pair(hidden, 6), cross(7), cross(6), cross(5), cross(4),
                 pair(grads, 6), pair(grads, 4), cross(3), cross(2), cross(1), cross(0), pair(grads, 2), pair(grads, 0)]
        packed, update, dsum = reduce_units(jnp.concatenate(units, axis=0), a_pre, s_pre, jnp.stack(diags))
        a_new, update = blend(packed, dsum, a_prev, 0, lambda t: t, update)
        s_new, = blend(packed, dsum, s_prev, 4, lambda t: 3 - t)
        return update, a_new, s_new

    return jax.shard_map(per_device, mesh=mesh, in_specs=(row_spec, row_spec) + (full_spec,) * 5, out_specs=(full_spec,) * 3, check_vma=False)
```

```python
import functools

import jax
import jax.numpy as jnp
from jax import lax
from jax.experimental import pallas as pl
from jax.experimental.pallas import tpu as pltpu
from jax.sharding import PartitionSpec as P

FACTOR_DECAY = 0.8
GELU_SCALE = 0.7978845608028654
GELU_CUBIC = 0.044715
MESH = pl.DeviceIdType.MESH
W = 768
ROUNDS = 8
NX, NR, NG = 3, 3, 4
PERIODS = ROUNDS + 5
DIAG_PERIOD = 7
BATCH = 1024
FWD, BWD = 512, 512
HIDDEN = 8
BF16 = jnp.bfloat16
F32 = jnp.float32
ALL = pl.ds(0, W)
SCALE = 1.0 / 131072.0


def comm_kernel(tok_ref, dout_ref, w_ref, ainv_ref, sinv_ref, packed_ref, upd_ref, dsum_ref,
                X, R, G, D, Y, ACT, WB, INV, UPD, MS, ML,
                rsem, ssem, dsend, drecv, isem, osem, osend, orecv, msend, mrecv, mloc, wsem, tsem):
    node, data = lax.axis_index('node'), lax.axis_index('data')
    core = lax.rem(data, 2)
    coord = [data // 2, lax.rem(node, 4), node // 4]

    def device(axis, delta):
        c = list(coord)
        c[axis] = lax.rem(c[axis] + delta + 4, 4)
        return (c[2] * 4 + c[1], c[0] * 2 + core)

    partner = (node, data + 1 - 2 * core)

    barrier = pltpu.get_barrier_semaphore()
    peers = [partner] + [device(a, d) for a in range(3) for d in (1, 2, 3)]
    for dev in peers:
        pl.semaphore_signal(barrier, inc=1, device_id=dev, device_id_type=MESH)
    pl.semaphore_wait(barrier, len(peers))

    def mo(v, m):
        return pl.multiple_of(v, m)

    def send(src, dst, s, r, dev):
        pltpu.make_async_remote_copy(src_ref=src, dst_ref=dst, send_sem=s, recv_sem=r, device_id=dev, device_id_type=MESH).start()

    def wait(ref, sem):
        pltpu.make_async_copy(ref, ref, sem).wait()

    def is_update(p):
        return (p >= 2) & (p < 6)

    def layer_of(p):
        return 11 - 2 * p - core

    def packed_of(p):
        return 2 * jnp.where(p < 2, p, p - 4) + core

    def place(k, s):
        return coord[(k + s) % 3]

    def region(p, k, s, j, half=None, slots=NX):
        row = mo(lax.rem(p, slots) * W, W) + 256 * k
        if s == 0:
            row = row + 64 * j
            n, col, m = 64, 0, W
        elif s == 1:
            row = row + 64 * place(k, 0) + 16 * j
            n, col, m = 16, 0, W
        else:
            row = row + 64 * place(k, 0) + 16 * place(k, 1) + 8 * (j // 2)
            n, col, m = 8, 384 * lax.rem(j, 2), 384
        if half is not None:
            if s < 2:
                n //= 2
                row = row + half * n
            else:
                col, m = (col, 128) if half == 0 else (col + 128, 256)
        row = mo(row, 8)
        if s < 2:
            return pl.ds(row, n), ALL
        return pl.ds(row, n), pl.ds(mo(col, 128), m)

    def landing(p, k, s, what, side=None, half=None):
        row = mo(lax.rem(p, NR) * W, W) + 256 * k
        if s < 2:
            h = (32, 8)[s]
            if side is None:
                start, n = 2 * what, 2 + 2 * what
            elif what == 0:
                start, n = side, 1
            elif half is None:
                start, n = 2 + 2 * side, 2
            else:
                start, n = 2 + 2 * side + half, 1
            return pl.ds(mo(row + 192 * s + start * h, 8), n * h), ALL
        row = pl.ds(mo(row + 240 + 8 * what, 8), 8)
        if side is None:
            return row, pl.ds(0, 384 * (1 + what))
        if what == 0:
            return row, pl.ds(128 * side, 128 * (side + 1))
        if half is None:
            return row, pl.ds(384 * side, 384)
        return row, pl.ds(384 * side + 128 * half, 128 * (half + 1))

    def neighbours(k, s):
        a = (k + s) % 3
        return place(k, s), device(a, 1), device(a, -1)

    def around(i):
        return lax.rem(i + 1, 4), lax.rem(i + 3, 4), lax.rem(i + 2, 4)

    def rs(p, k, s, w):
        return rsem.at[lax.rem(p, NR), (k * 3 + s) * 4 + w]

    def ss(p, k, s, w):
        return ssem.at[lax.rem(p, NR), (k * 3 + s) * 4 + w]

    def add(dst, src):
        X[dst] = X[dst] + R[src]

    def scatter_a(p, k, s):
        i, plus, minus = neighbours(k, s)
        jp, jm, j2 = around(i)
        fwd, blk, sa = rs(p, k, s, 0), rs(p, k, s, 1), ss(p, k, s, 0)
        send(X.at[region(p, k, s, j2, 0)], R.at[landing(p, k, s, 0, 0)], sa, fwd, minus)
        send(X.at[region(p, k, s, j2, 1)], R.at[landing(p, k, s, 0, 1)], sa, fwd, plus)
        send(X.at[region(p, k, s, jm, 1)], R.at[landing(p, k, s, 1, 0, 1)], sa, blk, minus)
        send(X.at[region(p, k, s, jp, 0)], R.at[landing(p, k, s, 1, 1, 0)], sa, blk, plus)

    def scatter_b(p, k, s):
        i, plus, minus = neighbours(k, s)
        jp, jm, _ = around(i)
        blk, sb = rs(p, k, s, 1), ss(p, k, s, 1)
        wait(R.at[landing(p, k, s, 0)], rs(p, k, s, 0))
        add(region(p, k, s, jm, 0), landing(p, k, s, 0, 0))
        send(X.at[region(p, k, s, jm, 0)], R.at[landing(p, k, s, 1, 0, 0)], sb, blk, minus)
        add(region(p, k, s, jp, 1), landing(p, k, s, 0, 1))
        send(X.at[region(p, k, s, jp, 1)], R.at[landing(p, k, s, 1, 1, 1)], sb, blk, plus)

    def scatter_c(p, k, s):
        i = place(k, s)
        wait(R.at[landing(p, k, s, 1)], rs(p, k, s, 1))
        mine = region(p, k, s, i)
        value = X[mine] + (R[landing(p, k, s, 1, 0)] + R[landing(p, k, s, 1, 1)])
        if s < 2:
            X[mine] = value
        else:
            G[region(p, k, s, i, slots=NG)] = value

    def gather_a(p, k, s):
        i, plus, minus = neighbours(k, s)
        mine = G.at[region(p, k, s, i, slots=NG)]
        send(mine, mine, ss(p, k, s, 2), rs(p, k, s, 2), plus)
        send(mine, mine, ss(p, k, s, 2), rs(p, k, s, 2), minus)

    def gather_b(p, k, s):
        i, plus, minus = neighbours(k, s)
        jp, jm, _ = around(i)
        wait(R.at[landing(p, k, s, 1)], rs(p, k, s, 2))
        from_minus, from_plus = G.at[region(p, k, s, jm, 0, slots=NG)], G.at[region(p, k, s, jp, 1, slots=NG)]
        send(from_minus, from_minus, ss(p, k, s, 3), rs(p, k, s, 3), plus)
        send(from_plus, from_plus, ss(p, k, s, 3), rs(p, k, s, 3), minus)

    def gather_c(p, k, s):
        wait(R.at[landing(p, k, s, 0)], rs(p, k, s, 3))

    def colours(f, p, s):
        for k in range(3):
            f(p, k, s)

    def gslot(p):
        return G.at[pl.ds(mo(lax.rem(p, NG) * W, W), W)]

    def xslot(p):
        return X.at[pl.ds(mo(lax.rem(p, NX) * W, W), W)]

    def unit(ref, index):
        return ref.at[pl.ds(mo(index * W, W), W)]

    def dslot(p):
        return D.at[pl.ds(mo(lax.rem(p, 2) * W, W), W)]

    def produced(p, which):
        return mo((lax.rem(p, 2) * 2 + which) * W, W)

    def step0(p):
        send(Y.at[pl.ds(produced(p, 1 - core), W)], dslot(p), dsend.at[lax.rem(p, 2)], drecv.at[lax.rem(p, 2)], partner)

    def step1(p):
        wait(dslot(p), drecv.at[lax.rem(p, 2)])

        def some(c, carry):
            a = pl.ds(mo(lax.rem(p, NX) * W + c * 64, 64), 64)
            X[a, :] = Y[pl.ds(mo(produced(p, core) + c * 64, 64), 64), :] + D[pl.ds(mo(lax.rem(p, 2) * W + c * 64, 64), 64), :]
            return carry
        lax.fori_loop(0, 12, some, 0)
        colours(scatter_a, p, 0)

    def step2(p):
        colours(scatter_b, p, 0)
        wait(dslot(p), dsend.at[lax.rem(p, 2)])

    def step3(p):
        colours(scatter_c, p, 0)
        colours(scatter_a, p, 1)

    def step4(p):
        colours(scatter_b, p, 1)

    def step5(p):
        colours(scatter_c, p, 1)
        colours(scatter_a, p, 2)

    def step6(p):
        colours(scatter_b, p, 2)

    def step7(p):
        colours(scatter_c, p, 2)
        colours(gather_a, p, 2)

    def sent(p, w):
        for k in range(3):
            for s in range(3):
                wait(R.at[landing(p, k, s, 1)], ss(p, k, s, w))
                wait(R.at[landing(p, k, s, 0)], ss(p, k, s, w + 1))

    def step8(p):
        colours(gather_b, p, 2)
        sent(p, 0)

    def step9(p):
        colours(gather_c, p, 2)
        colours(gather_a, p, 1)

    def inverse(which):
        return INV.at[pl.ds(which * W, W)]

    def load_inverses(p):
        l = layer_of(p)
        pltpu.make_async_copy(ainv_ref.at[l], inverse(0), isem.at[0]).start()
        pltpu.make_async_copy(sinv_ref.at[l], inverse(1), isem.at[1]).start()

    def step10(p):
        colours(gather_b, p, 1)

    def step11(p):
        colours(gather_c, p, 1)
        colours(gather_a, p, 0)

    def step12(p):
        colours(gather_b, p, 0)

    def piece(p, part):
        @pl.when(is_update(p))
        def _():
            rows = 256 * part
            a = INV[pl.ds(rows, 256), :]
            g = G[pl.ds(mo(lax.rem(p, NG) * W, W), W), :]
            left = jnp.dot(a, g, precision=lax.Precision.HIGHEST, preferred_element_type=F32) * SCALE
            b = INV[pl.ds(W, W), :]
            here = pl.ds(rows, 256)
            UPD[here, :] = jnp.dot(left, b, precision=lax.Precision.HIGHEST, preferred_element_type=F32)
            out = upd_ref.at[layer_of(p), pl.ds(rows, 256)]
            pltpu.make_async_copy(UPD.at[here], out, osem.at[lax.rem(p, 2)]).start()
            send(UPD.at[here], out, osend.at[lax.rem(p, 2)], orecv.at[p], partner)

    def step13(p):
        colours(gather_c, p, 0)

        @pl.when(is_update(p))
        def _():
            wait(inverse(0), isem.at[0])
            wait(inverse(1), isem.at[1])

        @pl.when(jnp.logical_not(is_update(p)))
        def _():
            out = packed_ref.at[packed_of(p)]
            pltpu.make_async_copy(gslot(p), out, osem.at[lax.rem(p, 2)]).start()
            send(gslot(p), out, osend.at[lax.rem(p, 2)], orecv.at[p], partner)
        piece(p, 0)

    def step14(p):
        sent(p, 2)
        piece(p, 1)

    def step15(p):
        piece(p, 2)

        @pl.when(is_update(p) & is_update(p + 1))
        def _():
            load_inverses(p + 1)

    def step16(p):
        wait(xslot(p), osem.at[lax.rem(p, 2)])
        wait(xslot(p), osend.at[lax.rem(p, 2)])

    def step17(p):
        wait(xslot(p), orecv.at[p])

    steps = [step0, step1, step2, step3, step4, step5, step6, step7, step8, step9, step10, step11, step12, step13, step14, step15, step16, step17]
    slots = [(0, 6, 9, 12, 3, 15), (7, 10, 4, 1, 16, 13), (8, 5, 11, 2, 14, 17)]

    def ms(n):
        return pl.ds(8 * n, 8)

    def small_send(stage):
        if stage == 0:
            send(MS.at[ms(0)], ML.at[ms(0)], msend.at[0], mrecv.at[0], partner)
        else:
            for d in (1, 2, 3):
                n = 3 * stage - 3 + d
                send(MS.at[ms(stage)], ML.at[ms(n)], msend.at[n], mrecv.at[n], device(stage - 1, d))

    def small_take(stage):
        if stage == 0:
            wait(ML.at[ms(0)], mrecv.at[0])
            wait(ML.at[ms(0)], msend.at[0])
            MS[ms(1), :] = MS[ms(0), :] + ML[ms(0), :]
        else:
            n = 3 * stage - 3
            for d in (1, 2, 3):
                wait(ML.at[ms(n + d)], mrecv.at[n + d])
                wait(ML.at[ms(n + d)], msend.at[n + d])
            MS[ms(stage + 1), :] = (MS[ms(stage), :] + ML[ms(n + 2), :]) + (ML[ms(n + 1), :] + ML[ms(n + 3), :])

    def small0():
        small_send(0)

    def small4():
        small_take(3)
        store = pltpu.make_async_copy(MS.at[ms(4)], dsum_ref, mloc.at[0])
        store.start()
        store.wait()

    def small_mid(n):
        small_take(n - 1)
        small_send(n)

    small = [small0] + [functools.partial(small_mid, n) for n in (1, 2, 3)] + [small4]

    def rows_of(slot, c, n):
        return pl.ds(mo(slot * BATCH + c * n, n), n)

    def weight_load(q):
        l = jnp.where(q <= 7, q, 14 - q)
        return pltpu.make_async_copy(w_ref.at[l], WB.at[pl.ds(mo(lax.rem(q, 2) * W, W), W)], wsem.at[lax.rem(q, 2)])

    def weights(q):
        weight_load(q).wait()

        @pl.when(q < 13)
        def _():
            weight_load(q + 1).start()
        return pl.ds(mo(lax.rem(q, 2) * W, W), W)

    def forward(l):
        here = weights(l)

        def chunk(c, carry):
            h = rows_of(HIDDEN, c, FWD)
            z = jnp.dot(ACT[h, :], WB[here, :], preferred_element_type=F32).astype(BF16)
            ACT[rows_of(l, c, FWD), :] = z
            zf = z.astype(F32)
            t = jnp.tanh(GELU_SCALE * (zf + GELU_CUBIC * zf * zf * zf))
            ACT[h, :] = (0.5 * zf * (1.0 + t)).astype(BF16)
            return carry
        lax.fori_loop(0, BATCH // FWD, chunk, 0)

    def backward(l):
        here = weights(14 - l)

        def chunk(c, carry):
            dh = lax.dot_general(ACT[rows_of(l, c, BWD), :], WB[here, :], (((1,), (1,)), ((), ())), preferred_element_type=F32).astype(BF16)
            below = rows_of(l - 1, c, BWD)
            zf = ACT[below, :].astype(F32)
            t = jnp.tanh(GELU_SCALE * (zf + GELU_CUBIC * zf * zf * zf))
            ACT[rows_of(HIDDEN, c, BWD), :] = (0.5 * zf * (1.0 + t)).astype(BF16)
            slope = 0.5 * (1.0 + t) + 0.5 * zf * (1.0 - t * t) * GELU_SCALE * (1.0 + 3.0 * GELU_CUBIC * zf * zf)
            ACT[below, :] = (dh.astype(F32) * slope).astype(BF16)
            return carry
        lax.fori_loop(0, BATCH // BWD, chunk, 0)

    def gram(left, right, dst, lower, diag_row):
        val = lax.dot_general(ACT[rows_of(left, 0, BATCH), :], ACT[rows_of(right, 0, BATCH), :],
                              (((0,), (0,)), ((), ())), preferred_element_type=F32)
        out = pl.ds(dst, W)

        @pl.when(jnp.logical_not(lower))
        def _():
            Y[out, :] = val

        @pl.when(lower)
        def _():
            r = lax.broadcasted_iota(jnp.int32, (W, W), 0)
            q = lax.broadcasted_iota(jnp.int32, (W, W), 1)
            Y[out, :] = jnp.where(r > q, val, Y[out, :])
            MS[pl.ds(diag_row, 1), :] = jnp.sum(jnp.where(r == q, val, 0.0), axis=0, keepdims=True)

    tok_load = pltpu.make_async_copy(tok_ref, ACT.at[pl.ds(HIDDEN * BATCH, BATCH)], tsem.at[0])
    dout_load = pltpu.make_async_copy(dout_ref, ACT.at[pl.ds(7 * BATCH, BATCH)], tsem.at[1])

    def item(p, j):
        upd = is_update(p)
        is_a = p < 2
        pair = j // 2
        l_a = 4 * p + j
        l_g = 11 - 2 * p - j
        l_s = 30 - 4 * p - 2 * pair + lax.rem(j, 2)
        l = jnp.where(is_a, l_a, jnp.where(upd, l_g, l_s))

        @pl.when(is_a & (l > 0))
        def _():
            forward(l - 1)

        @pl.when(upd & (l > 0))
        def _():
            backward(l)

        @pl.when(upd & (l == 0))
        def _():
            tok_load.start()
            tok_load.wait()

        left = jnp.where(is_a | upd, HIDDEN, l)
        right = jnp.where(is_a, HIDDEN, l)
        which = jnp.where(upd, j, pair)
        diag_row = jnp.where(is_a, 2 * p, 2 * p - 8) + pair
        gram(left, right, produced(p, which), jnp.logical_not(upd) & (lax.rem(l, 2) == 1), jnp.where(upd, 0, diag_row))

    weight_load(0).start()
    tok_load.start()
    dout_load.start()
    load_inverses(2)
    tok_load.wait()
    dout_load.wait()

    def period(n_period, carry):
        t = n_period - 1
        for sub in range(3):
            for n in slots[sub]:
                p = t - n // 3

                @pl.when((p >= 0) & (p < ROUNDS))
                def _(n=n, p=p):
                    steps[n](p)
            for n in range(5):
                if n % 3 == sub:
                    pl.when(t == DIAG_PERIOD + n // 3)(small[n])

            @pl.when(t + 1 < ROUNDS)
            def _(sub=sub):
                if sub < 2:
                    item(t + 1, sub)
                else:
                    @pl.when(jnp.logical_not(is_update(t + 1)))
                    def _():
                        def more(j, carry):
                            item(t + 1, j)
                            return carry
                        lax.fori_loop(2, 4, more, 0)
        return carry

    lax.fori_loop(0, PERIODS + 1, period, 0)


def reduce_units(tok, dout, w, a_inv, s_inv):
    any_space = pl.BlockSpec(memory_space=pl.ANY)
    dma = pltpu.SemaphoreType.DMA
    return pl.pallas_call(
        comm_kernel,
        out_shape=(jax.ShapeDtypeStruct((8, W, W), F32), jax.ShapeDtypeStruct((8, W, W), F32), jax.ShapeDtypeStruct((8, W), F32)),
        in_specs=[any_space] * 5,
        out_specs=(any_space,) * 3,
        scratch_shapes=[
            pltpu.VMEM((NX * W, W), F32),
            pltpu.VMEM((NR * W, W), F32),
            pltpu.VMEM((NG * W, W), F32),
            pltpu.VMEM((2 * W, W), F32),
            pltpu.VMEM((4 * W, W), F32),
            pltpu.VMEM((9 * BATCH, W), BF16),
            pltpu.VMEM((2 * W, W), BF16),
            pltpu.VMEM((2 * W, W), F32),
            pltpu.VMEM((W, W), F32),
            pltpu.VMEM((40, W), F32),
            pltpu.VMEM((80, W), F32),
            dma((NR, 36)), dma((NR, 36)), *[dma((n,)) for n in (2, 2, 2, 2, 2, ROUNDS, 10, 10, 1, 2, 2)],
        ],
        compiler_params=pltpu.CompilerParams(collective_id=0, has_side_effects=True, vmem_limit_bytes=67043328),
        name='reduce_units',
    )(tok, dout, w, a_inv, s_inv)


def blend_kernel(p_ref, d_ref, a_ref, s_ref, u_ref, a_out, s_out, u_out):
    t, h = pl.program_id(0), pl.program_id(1)

    @pl.when(h == 0)
    def _():
        u_out[...] = u_ref[...]
    block = 128

    def write(old_ref, new_ref):
        for rb in range(W // block):
            rows = pl.ds(rb * block, block)
            here = p_ref[0, rows, :]
            turned = p_ref[0, :, rows].T
            r = lax.broadcasted_iota(jnp.int32, (block, W), 0) + rb * block
            c = lax.broadcasted_iota(jnp.int32, (block, W), 1)
            first = jnp.where(r <= c, here, turned)
            second = jnp.where(r == c, d_ref[pl.ds(t, 1), :], jnp.where(r < c, turned, here))
            value = jnp.where(h == 0, first, second) * SCALE
            new_ref[0, rows, :] = FACTOR_DECAY * old_ref[0, rows, :] + (1.0 - FACTOR_DECAY) * value
    pl.when(t < 4)(functools.partial(write, a_ref, a_out))
    pl.when(t >= 4)(functools.partial(write, s_ref, s_out))


def blend(packed, dsum, a_old, s_old, update):
    mat = functools.partial(pl.BlockSpec, (1, W, W))
    each = mat(lambda t, h: (t, 0, 0))
    a_spec = mat(lambda t, h: (jnp.where(t < 4, 2 * t + h, 7), 0, 0))
    s_spec = mat(lambda t, h: (jnp.where(t < 4, 6, 14 - 2 * t + h), 0, 0))
    shape = jax.ShapeDtypeStruct((8, W, W), F32)
    return pl.pallas_call(
        blend_kernel,
        grid=(8, 2),
        in_specs=[each, pl.BlockSpec((8, W), lambda t, h: (0, 0)), a_spec, s_spec, each],
        out_specs=(a_spec, s_spec, each),
        out_shape=(shape,) * 3,
        compiler_params=pltpu.CompilerParams(vmem_limit_bytes=60 * 1024 * 1024),
        name='blend',
    )(packed, dsum, a_old, s_old, update)


def solution(mesh):
    row_spec = P(('node', 'data'), None)
    full_spec = P()

    def per_device(tok, dout, w, a_prev, s_prev, a_pre, s_pre):
        packed, update, dsum = reduce_units(tok, dout, w, a_pre, s_pre)
        a_new, s_new, update = blend(packed, dsum, a_prev, s_prev, update)
        return update, a_new, s_new

    return jax.shard_map(per_device, mesh=mesh, in_specs=(row_spec, row_spec) + (full_spec,) * 5, out_specs=(full_spec,) * 3, check_vma=False)
```

```python
import functools

import jax
import jax.numpy as jnp
from jax import lax
from jax.experimental import pallas as pl
from jax.experimental.pallas import tpu as pltpu
from jax.sharding import PartitionSpec as P

FACTOR_DECAY = 0.8
GELU_SCALE = 0.7978845608028654
GELU_CUBIC = 0.044715
MESH = pl.DeviceIdType.MESH
W = 768
ROUNDS = 8
NX, NR, NG = 3, 3, 4
PERIODS = ROUNDS + 5
DIAG_PERIOD = 7
BATCH = 1024
FWD, BWD = 512, 512
HIDDEN = 8
BF16 = jnp.bfloat16
F32 = jnp.float32
ALL = pl.ds(0, W)
SCALE = 1.0 / 131072.0
HALF = 384


def comm_kernel(tok_ref, dout_ref, w_ref, ainv_ref, sinv_ref, packed_ref, upd_ref, dsum_ref,
                X, R, G, D, Y, ACT, WB, INV, UPD, MS, ML,
                rsem, ssem, dsend, drecv, isem, osem, osend, orecv, msend, mrecv, mloc, wsem, tsem):
    node, data = lax.axis_index('node'), lax.axis_index('data')
    core = lax.rem(data, 2)
    coord = [data // 2, lax.rem(node, 4), node // 4]

    def device(axis, delta):
        c = list(coord)
        c[axis] = lax.rem(c[axis] + delta + 4, 4)
        return (c[2] * 4 + c[1], c[0] * 2 + core)

    partner = (node, data + 1 - 2 * core)

    barrier = pltpu.get_barrier_semaphore()
    peers = [partner] + [device(a, d) for a in range(3) for d in (1, 2, 3)]
    for dev in peers:
        pl.semaphore_signal(barrier, inc=1, device_id=dev, device_id_type=MESH)
    pl.semaphore_wait(barrier, len(peers))

    def mo(v, m):
        return pl.multiple_of(v, m)

    def send(src, dst, s, r, dev):
        pltpu.make_async_remote_copy(src_ref=src, dst_ref=dst, send_sem=s, recv_sem=r, device_id=dev, device_id_type=MESH).start()

    def wait(ref, sem):
        pltpu.make_async_copy(ref, ref, sem).wait()

    def is_update(p):
        return (p >= 2) & (p < 6)

    def layer_of(p):
        return 11 - 2 * p - core

    def packed_of(p):
        return 2 * jnp.where(p < 2, p, p - 4) + core

    def place(k, s):
        return coord[(k + s) % 3]

    def region(p, k, s, j, half=None, slots=NX):
        row = mo(lax.rem(p, slots) * W, W) + 256 * k
        if s == 0:
            row = row + 64 * j
            n, col, m = 64, 0, W
        elif s == 1:
            row = row + 64 * place(k, 0) + 16 * j
            n, col, m = 16, 0, W
        else:
            row = row + 64 * place(k, 0) + 16 * place(k, 1) + 8 * (j // 2)
            n, col, m = 8, 384 * lax.rem(j, 2), 384
        if half is not None:
            if s < 2:
                n //= 2
                row = row + half * n
            else:
                col, m = (col, 128) if half == 0 else (col + 128, 256)
        row = mo(row, 8)
        if s < 2:
            return pl.ds(row, n), ALL
        return pl.ds(row, n), pl.ds(mo(col, 128), m)

    def landing(p, k, s, what, side=None, half=None):
        row = mo(lax.rem(p, NR) * W, W) + 256 * k
        if s < 2:
            h = (32, 8)[s]
            if side is None:
                start, n = 2 * what, 2 + 2 * what
            elif what == 0:
                start, n = side, 1
            elif half is None:
                start, n = 2 + 2 * side, 2
            else:
                start, n = 2 + 2 * side + half, 1
            return pl.ds(mo(row + 192 * s + start * h, 8), n * h), ALL
        row = pl.ds(mo(row + 240 + 8 * what, 8), 8)
        if side is None:
            return row, pl.ds(0, 384 * (1 + what))
        if what == 0:
            return row, pl.ds(128 * side, 128 * (side + 1))
        if half is None:
            return row, pl.ds(384 * side, 384)
        return row, pl.ds(384 * side + 128 * half, 128 * (half + 1))

    def neighbours(k, s):
        a = (k + s) % 3
        return place(k, s), device(a, 1), device(a, -1)

    def around(i):
        return lax.rem(i + 1, 4), lax.rem(i + 3, 4), lax.rem(i + 2, 4)

    def rs(p, k, s, w):
        return rsem.at[lax.rem(p, NR), (k * 3 + s) * 4 + w]

    def ss(p, k, s, w):
        return ssem.at[lax.rem(p, NR), (k * 3 + s) * 4 + w]

    def add(dst, src):
        X[dst] = X[dst] + R[src]

    def scatter_a(p, k, s):
        i, plus, minus = neighbours(k, s)
        jp, jm, j2 = around(i)
        fwd, blk, sa = rs(p, k, s, 0), rs(p, k, s, 1), ss(p, k, s, 0)
        send(X.at[region(p, k, s, j2, 0)], R.at[landing(p, k, s, 0, 0)], sa, fwd, minus)
        send(X.at[region(p, k, s, j2, 1)], R.at[landing(p, k, s, 0, 1)], sa, fwd, plus)
        send(X.at[region(p, k, s, jm, 1)], R.at[landing(p, k, s, 1, 0, 1)], sa, blk, minus)
        send(X.at[region(p, k, s, jp, 0)], R.at[landing(p, k, s, 1, 1, 0)], sa, blk, plus)

    def scatter_b(p, k, s):
        i, plus, minus = neighbours(k, s)
        jp, jm, _ = around(i)
        blk, sb = rs(p, k, s, 1), ss(p, k, s, 1)
        wait(R.at[landing(p, k, s, 0)], rs(p, k, s, 0))
        add(region(p, k, s, jm, 0), landing(p, k, s, 0, 0))
        send(X.at[region(p, k, s, jm, 0)], R.at[landing(p, k, s, 1, 0, 0)], sb, blk, minus)
        add(region(p, k, s, jp, 1), landing(p, k, s, 0, 1))
        send(X.at[region(p, k, s, jp, 1)], R.at[landing(p, k, s, 1, 1, 1)], sb, blk, plus)

    def scatter_c(p, k, s):
        i = place(k, s)
        wait(R.at[landing(p, k, s, 1)], rs(p, k, s, 1))
        mine = region(p, k, s, i)
        value = X[mine] + (R[landing(p, k, s, 1, 0)] + R[landing(p, k, s, 1, 1)])
        if s < 2:
            X[mine] = value
        else:
            G[region(p, k, s, i, slots=NG)] = value

    def gather_a(p, k, s):
        i, plus, minus = neighbours(k, s)
        mine = G.at[region(p, k, s, i, slots=NG)]
        send(mine, mine, ss(p, k, s, 2), rs(p, k, s, 2), plus)
        send(mine, mine, ss(p, k, s, 2), rs(p, k, s, 2), minus)

    def gather_b(p, k, s):
        i, plus, minus = neighbours(k, s)
        jp, jm, _ = around(i)
        wait(R.at[landing(p, k, s, 1)], rs(p, k, s, 2))
        from_minus, from_plus = G.at[region(p, k, s, jm, 0, slots=NG)], G.at[region(p, k, s, jp, 1, slots=NG)]
        send(from_minus, from_minus, ss(p, k, s, 3), rs(p, k, s, 3), plus)
        send(from_plus, from_plus, ss(p, k, s, 3), rs(p, k, s, 3), minus)

    def gather_c(p, k, s):
        wait(R.at[landing(p, k, s, 0)], rs(p, k, s, 3))

    def colours(f, p, s):
        for k in range(3):
            f(p, k, s)

    def gslot(p):
        return G.at[pl.ds(mo(lax.rem(p, NG) * W, W), W)]

    def xslot(p):
        return X.at[pl.ds(mo(lax.rem(p, NX) * W, W), W)]

    def unit(ref, index):
        return ref.at[pl.ds(mo(index * W, W), W)]

    def dslot(p):
        return D.at[pl.ds(mo(lax.rem(p, 2) * W, W), W)]

    def produced(p, which):
        return mo((lax.rem(p, 2) * 2 + which) * W, W)

    def step0(p):
        send(Y.at[pl.ds(produced(p, 1 - core), W)], dslot(p), dsend.at[lax.rem(p, 2)], drecv.at[lax.rem(p, 2)], partner)

    def step1(p):
        wait(dslot(p), drecv.at[lax.rem(p, 2)])

        for k in range(3):
            def some(c, carry, k=k):
                n = 256 * k + c * 64
                X[pl.ds(mo(lax.rem(p, NX) * W + n, 64), 64), :] = (
                    Y[pl.ds(mo(produced(p, core) + n, 64), 64), :] + D[pl.ds(mo(lax.rem(p, 2) * W + n, 64), 64), :])
                return carry
            lax.fori_loop(0, 4, some, 0)
            scatter_a(p, k, 0)

    def step2(p):
        colours(scatter_b, p, 0)
        wait(dslot(p), dsend.at[lax.rem(p, 2)])

    def step3(p):
        colours(scatter_c, p, 0)
        colours(scatter_a, p, 1)

    def step4(p):
        colours(scatter_b, p, 1)

    def step5(p):
        colours(scatter_c, p, 1)
        colours(scatter_a, p, 2)

    def step6(p):
        colours(scatter_b, p, 2)

    def step7(p):
        colours(scatter_c, p, 2)
        colours(gather_a, p, 2)

    def sent(p, w):
        for k in range(3):
            for s in range(3):
                wait(R.at[landing(p, k, s, 1)], ss(p, k, s, w))
                wait(R.at[landing(p, k, s, 0)], ss(p, k, s, w + 1))

    def step8(p):
        colours(gather_b, p, 2)
        sent(p, 0)

    def step9(p):
        colours(gather_c, p, 2)
        colours(gather_a, p, 1)

    def inverse(which):
        return INV.at[pl.ds(which * W, W)]

    def load_inverses(p):
        l = layer_of(p)
        pltpu.make_async_copy(ainv_ref.at[l], inverse(0), isem.at[0]).start()
        pltpu.make_async_copy(sinv_ref.at[l], inverse(1), isem.at[1]).start()

    def step10(p):
        colours(gather_b, p, 1)

    def step11(p):
        colours(gather_c, p, 1)
        colours(gather_a, p, 0)

    def step12(p):
        colours(gather_b, p, 0)

    def piece(p, part):
        @pl.when(is_update(p))
        def _():
            rows = 256 * part
            a = INV[pl.ds(rows, 256), :]
            g = G[pl.ds(mo(lax.rem(p, NG) * W, W), W), :]
            left = jnp.dot(a, g, precision=lax.Precision.HIGHEST, preferred_element_type=F32) * SCALE
            b = INV[pl.ds(W, W), :]
            here = pl.ds(rows, 256)
            UPD[here, :] = jnp.dot(left, b, precision=lax.Precision.HIGHEST, preferred_element_type=F32)
            out = upd_ref.at[layer_of(p), pl.ds(rows, 256)]
            pltpu.make_async_copy(UPD.at[here], out, osem.at[lax.rem(p, 2)]).start()
            send(UPD.at[here], out, osend.at[lax.rem(p, 2)], orecv.at[p], partner)

    def step13(p):
        colours(gather_c, p, 0)

        @pl.when(is_update(p))
        def _():
            wait(inverse(0), isem.at[0])
            wait(inverse(1), isem.at[1])

        @pl.when(jnp.logical_not(is_update(p)))
        def _():
            out = packed_ref.at[packed_of(p)]
            pltpu.make_async_copy(gslot(p), out, osem.at[lax.rem(p, 2)]).start()
            send(gslot(p), out, osend.at[lax.rem(p, 2)], orecv.at[p], partner)
        piece(p, 0)

    def step14(p):
        sent(p, 2)
        piece(p, 1)

    def step15(p):
        piece(p, 2)

        @pl.when(is_update(p) & is_update(p + 1))
        def _():
            load_inverses(p + 1)

    def step16(p):
        wait(xslot(p), osem.at[lax.rem(p, 2)])
        wait(xslot(p), osend.at[lax.rem(p, 2)])

    def step17(p):
        wait(xslot(p), orecv.at[p])

    steps = [step0, step1, step2, step3, step4, step5, step6, step7, step8, step9, step10, step11, step12, step13, step14, step15, step16, step17]
    slots = [(0, 6, 9, 12, 3, 15), (7, 10, 4, 1, 16, 13), (8, 5, 11, 2, 14, 17)]

    def ms(n):
        return pl.ds(8 * n, 8)

    def small_send(stage):
        if stage == 0:
            send(MS.at[ms(0)], ML.at[ms(0)], msend.at[0], mrecv.at[0], partner)
        else:
            for d in (1, 2, 3):
                n = 3 * stage - 3 + d
                send(MS.at[ms(stage)], ML.at[ms(n)], msend.at[n], mrecv.at[n], device(stage - 1, d))

    def small_take(stage):
        if stage == 0:
            wait(ML.at[ms(0)], mrecv.at[0])
            wait(ML.at[ms(0)], msend.at[0])
            MS[ms(1), :] = MS[ms(0), :] + ML[ms(0), :]
        else:
            n = 3 * stage - 3
            for d in (1, 2, 3):
                wait(ML.at[ms(n + d)], mrecv.at[n + d])
                wait(ML.at[ms(n + d)], msend.at[n + d])
            MS[ms(stage + 1), :] = (MS[ms(stage), :] + ML[ms(n + 2), :]) + (ML[ms(n + 1), :] + ML[ms(n + 3), :])

    def small0():
        small_send(0)

    def small4():
        small_take(3)
        store = pltpu.make_async_copy(MS.at[ms(4)], dsum_ref, mloc.at[0])
        store.start()
        store.wait()

    def small_mid(n):
        small_take(n - 1)
        small_send(n)

    small = [small0] + [functools.partial(small_mid, n) for n in (1, 2, 3)] + [small4]

    def rows_of(slot, c, n):
        return pl.ds(mo(slot * BATCH + c * n, n), n)

    def weight_load(q):
        l = jnp.where(q <= 7, q, 14 - q)
        return pltpu.make_async_copy(w_ref.at[l], WB.at[pl.ds(mo(lax.rem(q, 2) * W, W), W)], wsem.at[lax.rem(q, 2)])

    def weights(q):
        weight_load(q).wait()

        @pl.when(q < 13)
        def _():
            weight_load(q + 1).start()
        return pl.ds(mo(lax.rem(q, 2) * W, W), W)

    def forward(l):
        here = weights(l)

        def chunk(c, carry):
            h = rows_of(HIDDEN, c, FWD)
            z = jnp.dot(ACT[h, :], WB[here, :], preferred_element_type=F32).astype(BF16)
            ACT[rows_of(l, c, FWD), :] = z
            zf = z.astype(F32)
            t = jnp.tanh(GELU_SCALE * (zf + GELU_CUBIC * zf * zf * zf))
            ACT[h, :] = (0.5 * zf * (1.0 + t)).astype(BF16)
            return carry
        lax.fori_loop(0, BATCH // FWD, chunk, 0)

    def backward(l):
        here = weights(14 - l)

        def chunk(c, carry):
            dh = lax.dot_general(ACT[rows_of(l, c, BWD), :], WB[here, :], (((1,), (1,)), ((), ())), preferred_element_type=F32).astype(BF16)
            below = rows_of(l - 1, c, BWD)
            zf = ACT[below, :].astype(F32)
            t = jnp.tanh(GELU_SCALE * (zf + GELU_CUBIC * zf * zf * zf))
            ACT[rows_of(HIDDEN, c, BWD), :] = (0.5 * zf * (1.0 + t)).astype(BF16)
            slope = 0.5 * (1.0 + t) + 0.5 * zf * (1.0 - t * t) * GELU_SCALE * (1.0 + 3.0 * GELU_CUBIC * zf * zf)
            ACT[below, :] = (dh.astype(F32) * slope).astype(BF16)
            return carry
        lax.fori_loop(0, BATCH // BWD, chunk, 0)

    def gram(left, right, dst, lower, diag_row):
        val = lax.dot_general(ACT[rows_of(left, 0, BATCH), :], ACT[rows_of(right, 0, BATCH), :],
                              (((0,), (0,)), ((), ())), preferred_element_type=F32)
        out = pl.ds(dst, W)

        @pl.when(jnp.logical_not(lower))
        def _():
            Y[out, :] = val

        @pl.when(lower)
        def _():
            r = lax.broadcasted_iota(jnp.int32, (W, W), 0)
            q = lax.broadcasted_iota(jnp.int32, (W, W), 1)
            Y[out, :] = jnp.where(r > q, val, Y[out, :])
            MS[pl.ds(diag_row, 1), :] = jnp.sum(jnp.where(r == q, val, 0.0), axis=0, keepdims=True)

    tok_load = pltpu.make_async_copy(tok_ref, ACT.at[pl.ds(HIDDEN * BATCH, BATCH)], tsem.at[0])
    dout_load = pltpu.make_async_copy(dout_ref, ACT.at[pl.ds(7 * BATCH, BATCH)], tsem.at[1])

    def item(p, j):
        upd = is_update(p)
        is_a = p < 2
        pair = j // 2
        l_a = 4 * p + j
        l_g = 11 - 2 * p - j
        l_s = 30 - 4 * p - 2 * pair + lax.rem(j, 2)
        l = jnp.where(is_a, l_a, jnp.where(upd, l_g, l_s))

        @pl.when(is_a & (l > 0))
        def _():
            forward(l - 1)

        @pl.when(upd & (l == 7))
        def _():
            dout_load.wait()

        @pl.when(upd & (l > 0))
        def _():
            backward(l)

        @pl.when(upd & (l == 0))
        def _():
            tok_load.start()
            tok_load.wait()

        left = jnp.where(is_a | upd, HIDDEN, l)
        right = jnp.where(is_a, HIDDEN, l)
        which = jnp.where(upd, j, pair)
        diag_row = jnp.where(is_a, 2 * p, 2 * p - 8) + pair
        gram(left, right, produced(p, which), jnp.logical_not(upd) & (lax.rem(l, 2) == 1), jnp.where(upd, 0, diag_row))

    tok_load.start()
    weight_load(0).start()
    tok_load.wait()
    dout_load.start()
    load_inverses(2)

    def period(n_period, carry):
        t = n_period - 1
        for sub in range(3):
            for n in slots[sub]:
                p = t - n // 3

                @pl.when((p >= 0) & (p < ROUNDS))
                def _(n=n, p=p):
                    steps[n](p)
            for n in range(5):
                if n % 3 == sub:
                    pl.when(t == DIAG_PERIOD + n // 3)(small[n])

            @pl.when(t + 1 < ROUNDS)
            def _(sub=sub):
                upd = is_update(t + 1)
                if sub == 0:
                    @pl.when(jnp.logical_not(upd))
                    def _():
                        item(t + 1, 0)
                elif sub == 1:
                    item(t + 1, jnp.where(upd, 0, 1))
                else:
                    def more(j, carry):
                        item(t + 1, j)
                        return carry
                    lax.fori_loop(jnp.where(upd, 1, 2), jnp.where(upd, 2, 4), more, 0)
        return carry

    lax.fori_loop(0, PERIODS + 1, period, 0)


def reduce_units(tok, dout, w, a_inv, s_inv):
    any_space = pl.BlockSpec(memory_space=pl.ANY)
    dma = pltpu.SemaphoreType.DMA
    return pl.pallas_call(
        comm_kernel,
        out_shape=(jax.ShapeDtypeStruct((8, W, W), F32), jax.ShapeDtypeStruct((8, W, W), F32), jax.ShapeDtypeStruct((8, W), F32)),
        in_specs=[any_space] * 5,
        out_specs=(any_space,) * 3,
        scratch_shapes=[
            pltpu.VMEM((NX * W, W), F32),
            pltpu.VMEM((NR * W, W), F32),
            pltpu.VMEM((NG * W, W), F32),
            pltpu.VMEM((2 * W, W), F32),
            pltpu.VMEM((4 * W, W), F32),
            pltpu.VMEM((9 * BATCH, W), BF16),
            pltpu.VMEM((2 * W, W), BF16),
            pltpu.VMEM((2 * W, W), F32),
            pltpu.VMEM((W, W), F32),
            pltpu.VMEM((40, W), F32),
            pltpu.VMEM((80, W), F32),
            dma((NR, 36)), dma((NR, 36)), *[dma((n,)) for n in (2, 2, 2, 2, 2, ROUNDS, 10, 10, 1, 2, 2)],
        ],
        compiler_params=pltpu.CompilerParams(collective_id=0, has_side_effects=True, vmem_limit_bytes=67043328),
        name='reduce_units',
    )(tok, dout, w, a_inv, s_inv)


def blend_kernel(p_ref, d_ref, a_ref, s_ref, u_ref, a_out, s_out, u_out):
    t, h = pl.program_id(0), pl.program_id(1)
    u_out[...] = u_ref[...]
    block = 128

    def write(old_ref, new_ref):
        for rb in range(HALF // block):
            rows = pl.ds(rb * block, block)
            top = h * HALF + rb * block
            far = pl.ds(pl.multiple_of(top, block), block)
            here = p_ref[0, far, :]
            turned = p_ref[0, :, far].T
            r = lax.broadcasted_iota(jnp.int32, (block, W), 0) + top
            c = lax.broadcasted_iota(jnp.int32, (block, W), 1)
            first = jnp.where(r <= c, here, turned) * SCALE
            second = jnp.where(r == c, d_ref[pl.ds(t, 1), :], jnp.where(r < c, turned, here)) * SCALE
            new_ref[0, rows, :] = FACTOR_DECAY * old_ref[0, rows, :] + (1.0 - FACTOR_DECAY) * first
            new_ref[1, rows, :] = FACTOR_DECAY * old_ref[1, rows, :] + (1.0 - FACTOR_DECAY) * second
    pl.when(t < 4)(functools.partial(write, a_ref, a_out))
    pl.when(t >= 4)(functools.partial(write, s_ref, s_out))


def blend(packed, dsum, a_old, s_old, update):
    two = functools.partial(pl.BlockSpec, (2, HALF, W))
    u_spec = pl.BlockSpec((1, HALF, W), lambda t, h: (t, h, 0))
    a_spec = two(lambda t, h: (jnp.minimum(t, 3), jnp.where(t < 4, h, 1), 0))
    s_spec = two(lambda t, h: (jnp.minimum(7 - t, 3), jnp.where(t < 4, 0, h), 0))
    shape = jax.ShapeDtypeStruct((8, W, W), F32)
    return pl.pallas_call(
        blend_kernel,
        grid=(8, 2),
        in_specs=[pl.BlockSpec((1, W, W), lambda t, h: (t, 0, 0)), pl.BlockSpec((8, W), lambda t, h: (0, 0)), a_spec, s_spec, u_spec],
        out_specs=(a_spec, s_spec, u_spec),
        out_shape=(shape,) * 3,
        compiler_params=pltpu.CompilerParams(vmem_limit_bytes=60 * 1024 * 1024),
        name='blend',
    )(packed, dsum, a_old, s_old, update)


def solution(mesh):
    row_spec = P(('node', 'data'), None)
    full_spec = P()

    def per_device(tok, dout, w, a_prev, s_prev, a_pre, s_pre):
        packed, update, dsum = reduce_units(tok, dout, w, a_pre, s_pre)
        a_new, s_new, update = blend(packed, dsum, a_prev, s_prev, update)
        return update, a_new, s_new

    return jax.shard_map(per_device, mesh=mesh, in_specs=(row_spec, row_spec) + (full_spec,) * 5, out_specs=(full_spec,) * 3, check_vma=False)
```

```python
import functools

import jax
import jax.numpy as jnp
from jax import lax
from jax.experimental import pallas as pl
from jax.experimental.pallas import tpu as pltpu
from jax.sharding import PartitionSpec as P

FACTOR_DECAY = 0.8
GELU_SCALE = 0.7978845608028654
GELU_CUBIC = 0.044715
MESH = pl.DeviceIdType.MESH
W = 768
ROUNDS = 8
NX, NR, NG = 3, 3, 4
PERIODS = ROUNDS + 5
DIAG_PERIOD = 7
BATCH = 1024
FWD, BWD = 512, 512
HIDDEN = 8
BF16 = jnp.bfloat16
F32 = jnp.float32
ALL = pl.ds(0, W)
SCALE = 1.0 / 131072.0
HALF = 384


def comm_kernel(tok_ref, dout_ref, w_ref, ainv_ref, sinv_ref, packed_ref, upd_ref, dsum_ref,
                X, R, G, D, Y, ACT, WB, INV, UPD, MS, ML,
                rsem, ssem, dsend, drecv, isem, osem, osend, orecv, msend, mrecv, mloc, wsem, tsem):
    node, data = lax.axis_index('node'), lax.axis_index('data')
    core = lax.rem(data, 2)
    coord = [data // 2, lax.rem(node, 4), node // 4]

    def device(axis, delta):
        c = list(coord)
        c[axis] = lax.rem(c[axis] + delta + 4, 4)
        return (c[2] * 4 + c[1], c[0] * 2 + core)

    partner = (node, data + 1 - 2 * core)

    barrier = pltpu.get_barrier_semaphore()
    peers = [partner] + [device(a, d) for a in range(3) for d in (1, 2, 3)]
    for dev in peers:
        pl.semaphore_signal(barrier, inc=1, device_id=dev, device_id_type=MESH)
    pl.semaphore_wait(barrier, len(peers))

    def mo(v, m):
        return pl.multiple_of(v, m)

    def send(src, dst, s, r, dev):
        pltpu.make_async_remote_copy(src_ref=src, dst_ref=dst, send_sem=s, recv_sem=r, device_id=dev, device_id_type=MESH).start()

    def wait(ref, sem):
        pltpu.make_async_copy(ref, ref, sem).wait()

    def is_update(p):
        return (p >= 2) & (p < 6)

    def layer_of(p):
        return 11 - 2 * p - core

    def packed_of(p):
        return 2 * jnp.where(p < 2, p, p - 4) + core

    def place(k, s):
        return coord[(k + s) % 3]

    def region(p, k, s, j, half=None, slots=NX):
        row = mo(lax.rem(p, slots) * W, W) + 256 * k
        if s == 0:
            row = row + 64 * j
            n, col, m = 64, 0, W
        elif s == 1:
            row = row + 64 * place(k, 0) + 16 * j
            n, col, m = 16, 0, W
        else:
            row = row + 64 * place(k, 0) + 16 * place(k, 1) + 8 * (j // 2)
            n, col, m = 8, 384 * lax.rem(j, 2), 384
        if half is not None:
            if s < 2:
                n //= 2
                row = row + half * n
            else:
                col, m = (col, 128) if half == 0 else (col + 128, 256)
        row = mo(row, 8)
        if s < 2:
            return pl.ds(row, n), ALL
        return pl.ds(row, n), pl.ds(mo(col, 128), m)

    def landing(p, k, s, what, side=None, half=None):
        row = mo(lax.rem(p, NR) * W, W) + 256 * k
        if s < 2:
            h = (32, 8)[s]
            if side is None:
                start, n = 2 * what, 2 + 2 * what
            elif what == 0:
                start, n = side, 1
            elif half is None:
                start, n = 2 + 2 * side, 2
            else:
                start, n = 2 + 2 * side + half, 1
            return pl.ds(mo(row + 192 * s + start * h, 8), n * h), ALL
        row = pl.ds(mo(row + 240 + 8 * what, 8), 8)
        if side is None:
            return row, pl.ds(0, 384 * (1 + what))
        if what == 0:
            return row, pl.ds(128 * side, 128 * (side + 1))
        if half is None:
            return row, pl.ds(384 * side, 384)
        return row, pl.ds(384 * side + 128 * half, 128 * (half + 1))

    def neighbours(k, s):
        a = (k + s) % 3
        return place(k, s), device(a, 1), device(a, -1)

    def around(i):
        return lax.rem(i + 1, 4), lax.rem(i + 3, 4), lax.rem(i + 2, 4)

    def rs(p, k, s, w):
        return rsem.at[lax.rem(p, NR), (k * 3 + s) * 4 + w]

    def ss(p, k, s, w):
        return ssem.at[lax.rem(p, NR), (k * 3 + s) * 4 + w]

    def add(dst, src):
        X[dst] = X[dst] + R[src]

    def scatter_a(p, k, s):
        i, plus, minus = neighbours(k, s)
        jp, jm, j2 = around(i)
        fwd, blk, sa = rs(p, k, s, 0), rs(p, k, s, 1), ss(p, k, s, 0)
        if s == 2:
            send(X.at[region(p, k, s, jp)], R.at[landing(p, k, s, 1, 1)], sa, blk, plus)
            send(X.at[region(p, k, s, jm)], R.at[landing(p, k, s, 1, 0)], sa, blk, minus)
            send(X.at[region(p, k, s, j2)], R.at[landing(p, k, s, 0)], ss(p, k, s, 1), fwd, device((k + s) % 3, 2))
            return
        send(X.at[region(p, k, s, j2, 0)], R.at[landing(p, k, s, 0, 0)], sa, fwd, minus)
        send(X.at[region(p, k, s, j2, 1)], R.at[landing(p, k, s, 0, 1)], sa, fwd, plus)
        send(X.at[region(p, k, s, jm, 1)], R.at[landing(p, k, s, 1, 0, 1)], sa, blk, minus)
        send(X.at[region(p, k, s, jp, 0)], R.at[landing(p, k, s, 1, 1, 0)], sa, blk, plus)

    def scatter_b(p, k, s):
        i, plus, minus = neighbours(k, s)
        jp, jm, _ = around(i)
        blk, sb = rs(p, k, s, 1), ss(p, k, s, 1)
        wait(R.at[landing(p, k, s, 0)], rs(p, k, s, 0))
        add(region(p, k, s, jm, 0), landing(p, k, s, 0, 0))
        send(X.at[region(p, k, s, jm, 0)], R.at[landing(p, k, s, 1, 0, 0)], sb, blk, minus)
        add(region(p, k, s, jp, 1), landing(p, k, s, 0, 1))
        send(X.at[region(p, k, s, jp, 1)], R.at[landing(p, k, s, 1, 1, 1)], sb, blk, plus)

    def scatter_c(p, k, s):
        i = place(k, s)
        wait(R.at[landing(p, k, s, 1)], rs(p, k, s, 1))
        mine = region(p, k, s, i)
        value = X[mine] + (R[landing(p, k, s, 1, 0)] + R[landing(p, k, s, 1, 1)])
        if s < 2:
            X[mine] = value
        else:
            wait(R.at[landing(p, k, s, 0)], rs(p, k, s, 0))
            value = value + R[landing(p, k, s, 0)]
            G[region(p, k, s, i, slots=NG)] = value

    def gather_a(p, k, s):
        i, plus, minus = neighbours(k, s)
        mine = G.at[region(p, k, s, i, slots=NG)]
        send(mine, mine, ss(p, k, s, 2), rs(p, k, s, 2), plus)
        send(mine, mine, ss(p, k, s, 2), rs(p, k, s, 2), minus)
        if s == 2:
            send(mine, mine, ss(p, k, s, 3), rs(p, k, s, 3), device((k + s) % 3, 2))

    def gather_b(p, k, s):
        i, plus, minus = neighbours(k, s)
        jp, jm, _ = around(i)
        wait(R.at[landing(p, k, s, 1)], rs(p, k, s, 2))
        from_minus, from_plus = G.at[region(p, k, s, jm, 0, slots=NG)], G.at[region(p, k, s, jp, 1, slots=NG)]
        send(from_minus, from_minus, ss(p, k, s, 3), rs(p, k, s, 3), plus)
        send(from_plus, from_plus, ss(p, k, s, 3), rs(p, k, s, 3), minus)

    def gather_c(p, k, s):
        if s == 2:
            wait(R.at[landing(p, k, s, 1)], rs(p, k, s, 2))
        wait(R.at[landing(p, k, s, 0)], rs(p, k, s, 3))

    def colours(f, p, s):
        for k in range(3):
            f(p, k, s)

    def gslot(p):
        return G.at[pl.ds(mo(lax.rem(p, NG) * W, W), W)]

    def xslot(p):
        return X.at[pl.ds(mo(lax.rem(p, NX) * W, W), W)]

    def unit(ref, index):
        return ref.at[pl.ds(mo(index * W, W), W)]

    def dslot(p):
        return D.at[pl.ds(mo(lax.rem(p, 2) * W, W), W)]

    def produced(p, which):
        return mo((lax.rem(p, 2) * 2 + which) * W, W)

    def step0(p):
        send(Y.at[pl.ds(produced(p, 1 - core), W)], dslot(p), dsend.at[lax.rem(p, 2)], drecv.at[lax.rem(p, 2)], partner)

    def step1(p):
        wait(dslot(p), drecv.at[lax.rem(p, 2)])

        for k in range(3):
            def some(c, carry, k=k):
                n = 256 * k + c * 64
                X[pl.ds(mo(lax.rem(p, NX) * W + n, 64), 64), :] = (
                    Y[pl.ds(mo(produced(p, core) + n, 64), 64), :] + D[pl.ds(mo(lax.rem(p, 2) * W + n, 64), 64), :])
                return carry
            lax.fori_loop(0, 4, some, 0)
            scatter_a(p, k, 0)

    def step2(p):
        colours(scatter_b, p, 0)
        wait(dslot(p), dsend.at[lax.rem(p, 2)])

    def step3(p):
        colours(scatter_c, p, 0)
        colours(scatter_a, p, 1)

    def step4(p):
        colours(scatter_b, p, 1)

    def step5(p):
        colours(scatter_c, p, 1)
        colours(scatter_a, p, 2)

    def step6(p):
        colours(scatter_c, p, 2)
        colours(gather_a, p, 2)

    def sent(p, w):
        for k in range(3):
            for s in range(3):
                wait(R.at[landing(p, k, s, 1)], ss(p, k, s, w))
                wait(R.at[landing(p, k, s, 0)], ss(p, k, s, w + 1))

    def step7(p):
        colours(gather_c, p, 2)
        colours(gather_a, p, 1)

    def inverse(which):
        return INV.at[pl.ds(which * W, W)]

    def load_inverses(p):
        l = layer_of(p)
        pltpu.make_async_copy(ainv_ref.at[l], inverse(0), isem.at[0]).start()
        pltpu.make_async_copy(sinv_ref.at[l], inverse(1), isem.at[1]).start()

    def step8(p):
        colours(gather_b, p, 1)
        sent(p, 0)

    def step9(p):
        colours(gather_c, p, 1)
        colours(gather_a, p, 0)

    def step10(p):
        colours(gather_b, p, 0)

    def piece(p, part):
        @pl.when(is_update(p))
        def _():
            rows = 256 * part
            a = INV[pl.ds(rows, 256), :]
            g = G[pl.ds(mo(lax.rem(p, NG) * W, W), W), :]
            left = jnp.dot(a, g, precision=lax.Precision.HIGHEST, preferred_element_type=F32) * SCALE
            b = INV[pl.ds(W, W), :]
            here = pl.ds(rows, 256)
            UPD[here, :] = jnp.dot(left, b, precision=lax.Precision.HIGHEST, preferred_element_type=F32)
            out = upd_ref.at[layer_of(p), pl.ds(rows, 256)]
            pltpu.make_async_copy(UPD.at[here], out, osem.at[lax.rem(p, 2)]).start()
            send(UPD.at[here], out, osend.at[lax.rem(p, 2)], orecv.at[p], partner)

    def step11(p):
        colours(gather_c, p, 0)

        @pl.when(is_update(p))
        def _():
            wait(inverse(0), isem.at[0])
            wait(inverse(1), isem.at[1])

        @pl.when(jnp.logical_not(is_update(p)))
        def _():
            out = packed_ref.at[packed_of(p)]
            pltpu.make_async_copy(gslot(p), out, osem.at[lax.rem(p, 2)]).start()
            send(gslot(p), out, osend.at[lax.rem(p, 2)], orecv.at[p], partner)
        piece(p, 0)

    def step12(p):
        sent(p, 2)
        piece(p, 1)

    def step13(p):
        piece(p, 2)

        @pl.when(is_update(p) & is_update(p + 1))
        def _():
            load_inverses(p + 1)

    def step14(p):
        wait(xslot(p), osem.at[lax.rem(p, 2)])
        wait(xslot(p), osend.at[lax.rem(p, 2)])

    def step15(p):
        wait(xslot(p), orecv.at[p])

    steps = [step0, step1, step2, step3, step4, step5, step6, step7, step8, step9, step10, step11, step12, step13, step14, step15]
    slots = [(0, 6, 9, 3, 12, 15), (7, 4, 1, 10, 13), (8, 5, 2, 14, 11)]

    def ms(n):
        return pl.ds(8 * n, 8)

    def small_send(stage):
        if stage == 0:
            send(MS.at[ms(0)], ML.at[ms(0)], msend.at[0], mrecv.at[0], partner)
        else:
            for d in (1, 2, 3):
                n = 3 * stage - 3 + d
                send(MS.at[ms(stage)], ML.at[ms(n)], msend.at[n], mrecv.at[n], device(stage - 1, d))

    def small_take(stage):
        if stage == 0:
            wait(ML.at[ms(0)], mrecv.at[0])
            wait(ML.at[ms(0)], msend.at[0])
            MS[ms(1), :] = MS[ms(0), :] + ML[ms(0), :]
        else:
            n = 3 * stage - 3
            for d in (1, 2, 3):
                wait(ML.at[ms(n + d)], mrecv.at[n + d])
                wait(ML.at[ms(n + d)], msend.at[n + d])
            MS[ms(stage + 1), :] = (MS[ms(stage), :] + ML[ms(n + 2), :]) + (ML[ms(n + 1), :] + ML[ms(n + 3), :])

    def small0():
        small_send(0)

    def small4():
        small_take(3)
        store = pltpu.make_async_copy(MS.at[ms(4)], dsum_ref, mloc.at[0])
        store.start()
        store.wait()

    def small_mid(n):
        small_take(n - 1)
        small_send(n)

    small = [small0] + [functools.partial(small_mid, n) for n in (1, 2, 3)] + [small4]

    def rows_of(slot, c, n):
        return pl.ds(mo(slot * BATCH + c * n, n), n)

    def weight_load(q):
        l = jnp.where(q <= 7, q, 14 - q)
        return pltpu.make_async_copy(w_ref.at[l], WB.at[pl.ds(mo(lax.rem(q, 2) * W, W), W)], wsem.at[lax.rem(q, 2)])

    def weights(q):
        weight_load(q).wait()

        @pl.when(q < 13)
        def _():
            weight_load(q + 1).start()
        return pl.ds(mo(lax.rem(q, 2) * W, W), W)

    def forward(l):
        here = weights(l)

        def chunk(c, carry):
            h = rows_of(HIDDEN, c, FWD)
            z = jnp.dot(ACT[h, :], WB[here, :], preferred_element_type=F32).astype(BF16)
            ACT[rows_of(l, c, FWD), :] = z
            zf = z.astype(F32)
            t = jnp.tanh(GELU_SCALE * (zf + GELU_CUBIC * zf * zf * zf))
            ACT[h, :] = (0.5 * zf * (1.0 + t)).astype(BF16)
            return carry
        lax.fori_loop(0, BATCH // FWD, chunk, 0)

    def backward(l):
        here = weights(14 - l)

        def chunk(c, carry):
            dh = lax.dot_general(ACT[rows_of(l, c, BWD), :], WB[here, :], (((1,), (1,)), ((), ())), preferred_element_type=F32).astype(BF16)
            below = rows_of(l - 1, c, BWD)
            zf = ACT[below, :].astype(F32)
            t = jnp.tanh(GELU_SCALE * (zf + GELU_CUBIC * zf * zf * zf))
            ACT[rows_of(HIDDEN, c, BWD), :] = (0.5 * zf * (1.0 + t)).astype(BF16)
            slope = 0.5 * (1.0 + t) + 0.5 * zf * (1.0 - t * t) * GELU_SCALE * (1.0 + 3.0 * GELU_CUBIC * zf * zf)
            ACT[below, :] = (dh.astype(F32) * slope).astype(BF16)
            return carry
        lax.fori_loop(0, BATCH // BWD, chunk, 0)

    def gram(left, right, dst, lower, diag_row):
        val = lax.dot_general(ACT[rows_of(left, 0, BATCH), :], ACT[rows_of(right, 0, BATCH), :],
                              (((0,), (0,)), ((), ())), preferred_element_type=F32)
        out = pl.ds(dst, W)

        @pl.when(jnp.logical_not(lower))
        def _():
            Y[out, :] = val

        @pl.when(lower)
        def _():
            r = lax.broadcasted_iota(jnp.int32, (W, W), 0)
            q = lax.broadcasted_iota(jnp.int32, (W, W), 1)
            Y[out, :] = jnp.where(r > q, val, Y[out, :])
            MS[pl.ds(diag_row, 1), :] = jnp.sum(jnp.where(r == q, val, 0.0), axis=0, keepdims=True)

    tok_load = pltpu.make_async_copy(tok_ref, ACT.at[pl.ds(HIDDEN * BATCH, BATCH)], tsem.at[0])
    dout_load = pltpu.make_async_copy(dout_ref, ACT.at[pl.ds(7 * BATCH, BATCH)], tsem.at[1])

    def item(p, j):
        upd = is_update(p)
        is_a = p < 2
        pair = j // 2
        l_a = 4 * p + j
        l_g = 11 - 2 * p - j
        l_s = 30 - 4 * p - 2 * pair + lax.rem(j, 2)
        l = jnp.where(is_a, l_a, jnp.where(upd, l_g, l_s))

        @pl.when(is_a & (l > 0))
        def _():
            forward(l - 1)

        @pl.when(upd & (l == 7))
        def _():
            dout_load.wait()

        @pl.when(upd & (l > 0))
        def _():
            backward(l)

        @pl.when(upd & (l == 0))
        def _():
            tok_load.start()
            tok_load.wait()

        left = jnp.where(is_a | upd, HIDDEN, l)
        right = jnp.where(is_a, HIDDEN, l)
        which = jnp.where(upd, j, pair)
        diag_row = jnp.where(is_a, 2 * p, 2 * p - 8) + pair
        gram(left, right, produced(p, which), jnp.logical_not(upd) & (lax.rem(l, 2) == 1), jnp.where(upd, 0, diag_row))

    tok_load.start()
    weight_load(0).start()
    tok_load.wait()
    dout_load.start()
    load_inverses(2)

    def period(n_period, carry):
        t = n_period - 1
        for sub in range(3):
            for n in slots[sub]:
                p = t - n // 3

                @pl.when((p >= 0) & (p < ROUNDS))
                def _(n=n, p=p):
                    steps[n](p)
            for n in range(5):
                if n % 3 == sub:
                    pl.when(t == DIAG_PERIOD + n // 3)(small[n])

            @pl.when(t + 1 < ROUNDS)
            def _(sub=sub):
                upd = is_update(t + 1)
                if sub == 0:
                    @pl.when(jnp.logical_not(upd))
                    def _():
                        item(t + 1, 0)
                elif sub == 1:
                    def more(j, carry):
                        item(t + 1, j)
                        return carry
                    lax.fori_loop(jnp.where(upd, 0, 1), jnp.where(upd, 1, 3), more, 0)
                else:
                    item(t + 1, jnp.where(upd, 1, 3))
        return carry

    lax.fori_loop(0, PERIODS + 1, period, 0)


def reduce_units(tok, dout, w, a_inv, s_inv):
    any_space = pl.BlockSpec(memory_space=pl.ANY)
    dma = pltpu.SemaphoreType.DMA
    return pl.pallas_call(
        comm_kernel,
        out_shape=(jax.ShapeDtypeStruct((8, W, W), F32), jax.ShapeDtypeStruct((8, W, W), F32), jax.ShapeDtypeStruct((8, W), F32)),
        in_specs=[any_space] * 5,
        out_specs=(any_space,) * 3,
        scratch_shapes=[
            pltpu.VMEM((NX * W, W), F32),
            pltpu.VMEM((NR * W, W), F32),
            pltpu.VMEM((NG * W, W), F32),
            pltpu.VMEM((2 * W, W), F32),
            pltpu.VMEM((4 * W, W), F32),
            pltpu.VMEM((9 * BATCH, W), BF16),
            pltpu.VMEM((2 * W, W), BF16),
            pltpu.VMEM((2 * W, W), F32),
            pltpu.VMEM((W, W), F32),
            pltpu.VMEM((40, W), F32),
            pltpu.VMEM((80, W), F32),
            dma((NR, 36)), dma((NR, 36)), *[dma((n,)) for n in (2, 2, 2, 2, 2, ROUNDS, 10, 10, 1, 2, 2)],
        ],
        compiler_params=pltpu.CompilerParams(collective_id=0, has_side_effects=True, vmem_limit_bytes=67043328),
        name='reduce_units',
    )(tok, dout, w, a_inv, s_inv)


def blend_kernel(p_ref, d_ref, a_ref, s_ref, u_ref, a_out, s_out, u_out):
    t, h = pl.program_id(0), pl.program_id(1)
    u_out[...] = u_ref[...]
    block = 128

    def write(old_ref, new_ref):
        for rb in range(HALF // block):
            rows = pl.ds(rb * block, block)
            top = h * HALF + rb * block
            far = pl.ds(pl.multiple_of(top, block), block)
            here = p_ref[0, far, :]
            turned = p_ref[0, :, far].T
            r = lax.broadcasted_iota(jnp.int32, (block, W), 0) + top
            c = lax.broadcasted_iota(jnp.int32, (block, W), 1)
            first = jnp.where(r <= c, here, turned) * SCALE
            second = jnp.where(r == c, d_ref[pl.ds(t, 1), :], jnp.where(r < c, turned, here)) * SCALE
            new_ref[0, rows, :] = FACTOR_DECAY * old_ref[0, rows, :] + (1.0 - FACTOR_DECAY) * first
            new_ref[1, rows, :] = FACTOR_DECAY * old_ref[1, rows, :] + (1.0 - FACTOR_DECAY) * second
    pl.when(t < 4)(functools.partial(write, a_ref, a_out))
    pl.when(t >= 4)(functools.partial(write, s_ref, s_out))


def blend(packed, dsum, a_old, s_old, update):
    two = functools.partial(pl.BlockSpec, (2, HALF, W))
    u_spec = pl.BlockSpec((1, HALF, W), lambda t, h: (t, h, 0))
    a_spec = two(lambda t, h: (jnp.minimum(t, 3), jnp.where(t < 4, h, 1), 0))
    s_spec = two(lambda t, h: (jnp.minimum(7 - t, 3), jnp.where(t < 4, 0, h), 0))
    shape = jax.ShapeDtypeStruct((8, W, W), F32)
    return pl.pallas_call(
        blend_kernel,
        grid=(8, 2),
        in_specs=[pl.BlockSpec((1, W, W), lambda t, h: (t, 0, 0)), pl.BlockSpec((8, W), lambda t, h: (0, 0)), a_spec, s_spec, u_spec],
        out_specs=(a_spec, s_spec, u_spec),
        out_shape=(shape,) * 3,
        compiler_params=pltpu.CompilerParams(vmem_limit_bytes=60 * 1024 * 1024),
        name='blend',
    )(packed, dsum, a_old, s_old, update)


def solution(mesh):
    row_spec = P(('node', 'data'), None)
    full_spec = P()

    def per_device(tok, dout, w, a_prev, s_prev, a_pre, s_pre):
        packed, update, dsum = reduce_units(tok, dout, w, a_pre, s_pre)
        a_new, s_new, update = blend(packed, dsum, a_prev, s_prev, update)
        return update, a_new, s_new

    return jax.shard_map(per_device, mesh=mesh, in_specs=(row_spec, row_spec) + (full_spec,) * 5, out_specs=(full_spec,) * 3, check_vma=False)
```
